8 devices in a mesh: batch: 2 (over z, y), seq: 4 (over x, core).
Axes of the slice: x: 2, y: 2, z: 1, core: 2. Of those that a mesh axis runs over, the one named last changes fastest.
Arguments:
- hidden: bfloat16 [64, 4, 6144], P('batch'), parts along dimension 0
- cache_lens: int32 [64], P('batch'), parts along dimension 0
- c_kv: bfloat16 [64, 16384, 512], P('batch', 'seq'), parts along dimension 0
- k_r: bfloat16 [64, 16384, 64], P('batch', 'seq'), parts along dimension 0
- w_uq: bfloat16 [6144, 64, 128], P(None, 'seq')
- w_qr: bfloat16 [6144, 64, 64], P(None, 'seq')
- w_uk: bfloat16 [64, 128, 512], P('seq')
- w_uv: bfloat16 [64, 512, 128], P('seq')
- w_o: bfloat16 [64, 128, 6144], P('seq')
Outputs:
- output: bfloat16 [64, 4, 6144], P('batch'), parts along dimension 0
There are 2 independent parts. The reference program is written for one: setup_inputs(seed, part) draws one part's arguments, and reference() takes and returns one part's arrays. A program takes and returns all parts, laid end to end along the dimension named above; an argument that names none is the same for every part.
All inputs are finite; a program needn't handle non-finite values.
Results may differ from the reference program's by a relative error of at most 0.00663798.
Values are sent between devices in bfloat16 or wider.
A program may use at most 1 GiB of HBM per device.

```python
import jax
import jax.numpy as jnp
from jax import lax

ROW_COUNT = 32
CTX_LEN = 16384
Q_LEN = 4
MODEL_DIM = 6144
NUM_HEADS = 64
NOPE_DIM = 128
ROPE_DIM = 64
LATENT_DIM = 512
VALUE_DIM = 128


def setup_inputs(seed: int = 0, part: int = 0) -> dict:
    part_key = jax.random.fold_in(jax.random.key(seed), part)
    key_x, key_lens, key_cache, key_rope = jax.random.split(part_key, 4)
    key_uq, key_qr, key_uk, key_uv, key_wo = jax.random.split(jax.random.key(seed + 1), 5)
    hidden = jax.random.normal(key_x, (ROW_COUNT, Q_LEN, MODEL_DIM), jnp.float32)
    short_by = jax.random.randint(key_lens, (ROW_COUNT,), 0, CTX_LEN // 4 + 1)
    cache_lens = (CTX_LEN - Q_LEN - short_by).at[0].set(CTX_LEN - Q_LEN)
    c_kv = jax.random.normal(key_cache, (ROW_COUNT, CTX_LEN, LATENT_DIM), jnp.float32)
    k_r = jax.random.normal(key_rope, (ROW_COUNT, CTX_LEN, ROPE_DIM), jnp.float32)
    w_uq = jax.random.normal(key_uq, (MODEL_DIM, NUM_HEADS, NOPE_DIM), jnp.float32) * MODEL_DIM ** -0.5
    w_qr = jax.random.normal(key_qr, (MODEL_DIM, NUM_HEADS, ROPE_DIM), jnp.float32) * (2.0 * MODEL_DIM ** -0.5)
    w_uk = jax.random.normal(key_uk, (NUM_HEADS, NOPE_DIM, LATENT_DIM), jnp.float32) * (2.0 * NOPE_DIM ** -0.5)
    w_uv = jax.random.normal(key_uv, (NUM_HEADS, LATENT_DIM, VALUE_DIM), jnp.float32) * LATENT_DIM ** -0.5
    w_o = jax.random.normal(key_wo, (NUM_HEADS, VALUE_DIM, MODEL_DIM), jnp.float32) * (2.0 * (NUM_HEADS * VALUE_DIM) ** -0.5)
    return {
        "hidden": hidden.astype(jnp.bfloat16),
        "cache_lens": cache_lens.astype(jnp.int32),
        "c_kv": c_kv.astype(jnp.bfloat16),
        "k_r": k_r.astype(jnp.bfloat16),
        "w_uq": w_uq.astype(jnp.bfloat16),
        "w_qr": w_qr.astype(jnp.bfloat16),
        "w_uk": w_uk.astype(jnp.bfloat16),
        "w_uv": w_uv.astype(jnp.bfloat16),
        "w_o": w_o.astype(jnp.bfloat16),
    }


def reference(hidden, cache_lens, c_kv, k_r, w_uq, w_qr, w_uk, w_uv, w_o):
    hidden_wide = hidden.astype(jnp.float32)
    q_nope = jnp.einsum("bqd,dhk->bqhk", hidden_wide, w_uq.astype(jnp.float32)).astype(jnp.bfloat16)
    q_rope = jnp.einsum("bqd,dhr->bqhr", hidden_wide, w_qr.astype(jnp.float32)).astype(jnp.bfloat16)
    q_lat = jnp.einsum("bqhk,hkc->bqhc", q_nope.astype(jnp.float32), w_uk.astype(jnp.float32)).astype(jnp.bfloat16)
    score_scale = (NOPE_DIM + ROPE_DIM) ** -0.5
    positions = jnp.arange(CTX_LEN)
    offsets = jnp.arange(Q_LEN)

    def row_attend(row_args):
        lat_row, rope_row, cache_row, key_row, row_len = row_args
        cache_wide = cache_row.astype(jnp.float32)
        scores = (jnp.einsum("qhc,tc->qht", lat_row.astype(jnp.float32), cache_wide)
                  + jnp.einsum("qhr,tr->qht", rope_row.astype(jnp.float32), key_row.astype(jnp.float32))) * score_scale
        visible = positions[None, None, :] <= (row_len + offsets)[:, None, None]
        probs = jax.nn.softmax(jnp.where(visible, scores, -jnp.inf), axis=-1)
        return jnp.einsum("qht,tc->qhc", probs, cache_wide)

    o_lat = lax.map(row_attend, (q_lat, q_rope, c_kv, k_r, cache_lens)).astype(jnp.bfloat16)
    o_val = jnp.einsum("bqhc,hcv->bqhv", o_lat.astype(jnp.float32), w_uv.astype(jnp.float32)).astype(jnp.bfloat16)
    y_sum = jnp.einsum("bqhv,hvd->bqd", o_val.astype(jnp.float32), w_o.astype(jnp.float32))
    return (hidden_wide + y_sum).astype(jnp.bfloat16)
```

```python
import functools
import math

import jax
import jax.numpy as jnp
from jax import lax
from jax.experimental import pallas as pl
from jax.experimental.pallas import tpu as pltpu
from jax.sharding import PartitionSpec as P

MASK_FILL = -1e30
MESH = pl.DeviceIdType.MESH
CHUNK = 1024


def _attend_kernel(rows, toks, seq_len, score_scale, lens_ref, q_hbm, kv_hbm, kr_hbm, o_ref,
                   qbuf, kvbuf, krbuf, oacc, ostat, pbuf, pstat, xsend, xstat, xrecv, xrstat, own,
                   q_local, q_cross, q_side, q_fwd, kv_sem, kr_sem, p_sem, ps_sem, x_sem, xs_sem):
    me = lax.axis_index("seq")
    side = me + 1 - 2 * lax.rem(me, 2)
    cross = lax.rem(me + 2, 4)
    diag = lax.rem(side + 2, 4)
    pairs = rows // 2
    lat = kvbuf.shape[2]
    rope = kr_hbm.shape[1]
    group = qbuf.shape[2]
    queries = 4 * group

    def to(dev):
        return {"seq": dev}

    def kv_copies(row, slot):
        return (pltpu.make_async_copy(kv_hbm.at[row], kvbuf.at[slot], kv_sem.at[slot]),
                pltpu.make_async_copy(kr_hbm.at[row], krbuf.at[slot, pl.ds(pl.multiple_of(slot * rope, rope), rope)], kr_sem.at[slot]))

    def local_q(k):
        return pltpu.make_async_copy(q_hbm.at[k], qbuf.at[k, 0], q_local.at[k])

    def cross_q(k):
        return pltpu.make_async_remote_copy(q_hbm.at[k], qbuf.at[k, 1], q_cross.at[0, k], q_cross.at[1, k],
                                            device_id=to(cross), device_id_type=MESH)

    def side_q(k):
        return pltpu.make_async_remote_copy(q_hbm.at[k], qbuf.at[k, 2], q_side.at[0, k], q_side.at[1, k],
                                            device_id=to(side), device_id_type=MESH)

    def fwd_q(k):
        return pltpu.make_async_remote_copy(qbuf.at[k, 1], qbuf.at[k, 3], q_fwd.at[0, k], q_fwd.at[1, k],
                                            device_id=to(side), device_id_type=MESH)

    def side_o(row):
        slot, land = lax.rem(row, 2), lax.rem(row, 4)
        return (pltpu.make_async_remote_copy(oacc.at[slot, pl.ds(2 * group, 2 * group)], pbuf.at[land], p_sem.at[0, slot], p_sem.at[1, land],
                                             device_id=to(side), device_id_type=MESH),
                pltpu.make_async_remote_copy(ostat.at[slot, :, pl.ds(2 * group, 2 * group)], pstat.at[land], ps_sem.at[0, slot], ps_sem.at[1, land],
                                             device_id=to(side), device_id_type=MESH))

    def cross_o(row):
        return (pltpu.make_async_remote_copy(xsend.at[row], xrecv.at[row], x_sem.at[0, row], x_sem.at[1, row],
                                             device_id=to(cross), device_id_type=MESH),
                pltpu.make_async_remote_copy(xstat.at[row], xrstat.at[row], xs_sem.at[0, row], xs_sem.at[1, row],
                                             device_id=to(cross), device_id_type=MESH))

    for copy in kv_copies(0, 0):
        copy.start()
    local_q(0).start()
    barrier = pltpu.get_barrier_semaphore()
    for dev in (side, cross, diag):
        pl.semaphore_signal(barrier, inc=1, device_id=to(dev), device_id_type=MESH)
    pl.semaphore_wait(barrier, 3)

    def launch(k, carry):
        cross_q(k).start()
        side_q(k).start()

        @pl.when(k > 0)
        def _():
            local_q(k).start()
        return carry
    lax.fori_loop(0, pairs, launch, 0)
    krbuf[0, rope:, :] = jnp.zeros((rope, krbuf.shape[2]), krbuf.dtype)
    krbuf[1, :rope, :] = jnp.zeros((rope, krbuf.shape[2]), krbuf.dtype)

    def forward(k):
        cross_q(k).wait_recv()
        fwd_q(k).start()

    forward(0)
    fold = score_scale * math.log2(math.e)
    tok_of = lax.rem(lax.broadcasted_iota(jnp.int32, (queries, 1), 0), toks)
    lane_of = lax.broadcasted_iota(jnp.int32, (queries, CHUNK), 1)

    def attend(row, slot):
        pair = row // 2
        q_lat = qbuf[pair, :, :, pl.ds(pl.multiple_of(slot * lat, lat), lat)].reshape(queries, lat)
        q_rot = qbuf[pair, :, :, 2 * lat:].reshape(queries, 2 * rope)
        limit = lens_ref[row] - me * seq_len + tok_of
        top = total = acc = None
        for j in range(seq_len // CHUNK):
            part = kvbuf[slot, j * CHUNK:(j + 1) * CHUNK, :]
            s = lax.dot_general(q_lat, part, (((1,), (1,)), ((), ())), preferred_element_type=jnp.float32)
            s = s + jnp.dot(q_rot, krbuf[slot, :, j * CHUNK:(j + 1) * CHUNK], preferred_element_type=jnp.float32)
            s = jnp.where(lane_of <= limit - j * CHUNK, s * fold, MASK_FILL)
            peak = jnp.max(s, axis=1, keepdims=True)
            new_top = peak if top is None else jnp.maximum(top, peak)
            p = jnp.exp2(s - new_top)
            psum = jnp.sum(p, axis=1, keepdims=True)
            o = jnp.dot(p.astype(jnp.bfloat16), part, preferred_element_type=jnp.float32)
            if top is None:
                total, acc = psum, o
            else:
                keep = jnp.exp2(top - new_top)
                total = total * keep + psum
                acc = acc * keep + o
            top = new_top
        oacc[slot] = acc
        ostat[slot, 0] = jnp.broadcast_to(top, (queries, 128))
        ostat[slot, 1] = jnp.broadcast_to(total, (queries, 128))

    def merge_side(row):
        slot, land = lax.rem(row, 2), lax.rem(row, 4)
        for copy in side_o(row):
            copy.wait()
        top_a, top_b = ostat[slot, 0, :2 * group], pstat[land, 0]
        new_top = jnp.maximum(top_a, top_b)
        keep_a, keep_b = jnp.exp2(top_a - new_top), jnp.exp2(top_b - new_top)
        total = ostat[slot, 1, :2 * group] * keep_a + pstat[land, 1] * keep_b
        for n in range(lat // 128):
            cols = slice(n * 128, (n + 1) * 128)
            merged = oacc[slot, :2 * group, cols] * keep_a + pbuf[land, :, cols] * keep_b
            own[row, :, cols] = merged[:group]
            xsend[row, :, cols] = merged[group:]
        lane = lax.broadcasted_iota(jnp.int32, (2 * group, 128), 1)
        packed = jnp.transpose(jnp.where(lane == 0, new_top, total))
        xstat[row] = packed[:8]
        for copy in cross_o(row):
            copy.start()

    def body(row, carry):
        slot = lax.rem(row, 2)
        pair = row // 2

        @pl.when(row + 1 < rows)
        def _():
            for copy in kv_copies(row + 1, 1 - slot):
                copy.start()

        @pl.when(slot == 0)
        def _():
            local_q(pair).wait()
            side_q(pair).wait_recv()
            fwd_q(pair).wait_recv()

        @pl.when((slot == 1) & (pair + 1 < pairs))
        def _():
            forward(pair + 1)

        for copy in kv_copies(row, slot):
            copy.wait()
        attend(row, slot)
        for copy in side_o(row):
            copy.start()

        @pl.when(row > 0)
        def _():
            merge_side(row - 1)
        return carry

    lax.fori_loop(0, rows, body, 0)
    merge_side(rows - 1)

    def finish(row, carry):
        for copy in cross_o(row):
            copy.wait_recv()
        pad = jnp.zeros((120, 128), jnp.float32)
        mine = jnp.transpose(jnp.concatenate([xstat[row], pad], axis=0))[:group]
        theirs = jnp.transpose(jnp.concatenate([xrstat[row], pad], axis=0))[group:]
        top_a, top_b = mine[:, 0:1], theirs[:, 0:1]
        new_top = jnp.maximum(top_a, top_b)
        keep_a, keep_b = jnp.exp2(top_a - new_top), jnp.exp2(top_b - new_top)
        total = mine[:, 1:2] * keep_a + theirs[:, 1:2] * keep_b
        o_ref[row] = ((own[row] * keep_a + xrecv[row] * keep_b) / total).astype(o_ref.dtype)
        return carry
    lax.fori_loop(0, rows, finish, 0)

    def drain_q(k, carry):
        cross_q(k).wait_send()
        side_q(k).wait_send()
        fwd_q(k).wait_send()
        return carry
    lax.fori_loop(0, pairs, drain_q, 0)

    def drain_o(row, carry):
        for copy in cross_o(row):
            copy.wait_send()
        return carry
    lax.fori_loop(0, rows, drain_o, 0)


def _attend(lens, q_pack, c_kv, k_rt, toks, score_scale):
    rows, seq_len, lat = c_kv.shape
    rope = k_rt.shape[1]
    pairs, group, width = q_pack.shape
    f32, bf16 = jnp.float32, jnp.bfloat16
    dma = pltpu.SemaphoreType.DMA
    return pl.pallas_call(
        functools.partial(_attend_kernel, rows, toks, seq_len, score_scale),
        out_shape=jax.ShapeDtypeStruct((rows, group, lat), bf16),
        in_specs=[pl.BlockSpec(memory_space=pltpu.SMEM)] + [pl.BlockSpec(memory_space=pl.ANY)] * 3,
        out_specs=pl.BlockSpec(memory_space=pltpu.VMEM),
        scratch_shapes=[
            pltpu.VMEM((pairs, 4, group, width), bf16),
            pltpu.VMEM((2, seq_len, lat), bf16),
            pltpu.VMEM((2, 2 * rope, seq_len), bf16),
            pltpu.VMEM((2, 4 * group, lat), f32),
            pltpu.VMEM((2, 2, 4 * group, 128), f32),
            pltpu.VMEM((4, 2 * group, lat), f32),
            pltpu.VMEM((4, 2, 2 * group, 128), f32),
            pltpu.VMEM((rows, group, lat), f32),
            pltpu.VMEM((rows, 8, 128), f32),
            pltpu.VMEM((rows, group, lat), f32),
            pltpu.VMEM((rows, 8, 128), f32),
            pltpu.VMEM((rows, group, lat), f32),
            dma((pairs,)), dma((2, pairs)), dma((2, pairs)), dma((2, pairs)),
            dma((2,)), dma((2,)), dma((2, 4)), dma((2, 4)), dma((2, rows)), dma((2, rows)),
        ],
        compiler_params=pltpu.CompilerParams(collective_id=0, has_side_effects=True, vmem_limit_bytes=60 * 1024 * 1024),
        name="attend",
    )(lens, q_pack, c_kv, k_rt)


def solution(mesh):
    def local_step(hidden, cache_lens, c_kv, k_r, w_uq, w_qr, w_uk, w_uv, w_o):
        rows, toks, _ = hidden.shape
        heads, nope, lat = w_uk.shape
        rope = w_qr.shape[2]
        score_scale = (nope + rope) ** -0.5
        q_nope = jnp.einsum("cre,eil->cril", hidden, w_uq, preferred_element_type=jnp.float32).astype(jnp.bfloat16)
        q_rope = jnp.einsum("cre,eis->cris", hidden, w_qr, preferred_element_type=jnp.float32).astype(jnp.bfloat16)
        q_lat = jnp.einsum("bqhk,hkc->bqhc", q_nope, w_uk, preferred_element_type=jnp.float32).astype(jnp.bfloat16)
        q_lat = q_lat.reshape(rows // 2, 2, toks, heads, lat).transpose(0, 3, 2, 1, 4).reshape(rows // 2, heads * toks, 2 * lat)
        q_rope = q_rope.reshape(rows // 2, 2, toks, heads, rope).transpose(0, 3, 2, 1, 4).reshape(rows // 2, heads * toks, 2 * rope)
        q_pack = jnp.concatenate([q_lat, q_rope], axis=-1)
        o_lat = _attend(cache_lens, q_pack, c_kv, jnp.swapaxes(k_r, 1, 2), toks, score_scale)
        o_lat = o_lat.reshape(rows, heads, toks, lat).transpose(0, 2, 1, 3)
        o_val = jnp.einsum("bqhc,hcv->bqhv", o_lat, w_uv, preferred_element_type=jnp.float32).astype(jnp.bfloat16)
        y_part = jnp.einsum("criw,iwe->cre", o_val, w_o, preferred_element_type=jnp.float32)
        y_sum = lax.psum(y_part, "seq")
        return (hidden.astype(jnp.float32) + y_sum).astype(jnp.bfloat16)

    specs_in = (P("batch", None, None), P("batch"), P("batch", "seq", None), P("batch", "seq", None),
                P(None, "seq", None), P(None, "seq", None), P("seq", None, None), P("seq", None, None),
                P("seq", None, None))
    return jax.shard_map(local_step, mesh=mesh, in_specs=specs_in, out_specs=P("batch", None, None), check_vma=False)
```

```python
import functools
import math

import jax
import jax.numpy as jnp
from jax import lax
from jax.experimental import pallas as pl
from jax.experimental.pallas import tpu as pltpu
from jax.sharding import PartitionSpec as P

MASK_FILL = -1e30
MESH = pl.DeviceIdType.MESH
CHUNK = 1024


def _attend_kernel(rows, toks, seq_len, score_scale, lens_ref, q_hbm, kv_hbm, kr_hbm, o_ref,
                   qbuf, kvbuf, krbuf, oacc, ostat, pbuf, pstat, xsend, xstat, xrecv, xrstat, own,
                   q_local, q_cross, q_side, q_fwd, kv_sem, kr_sem, p_sem, ps_sem, x_sem, xs_sem):
    me = lax.axis_index("seq")
    side = me + 1 - 2 * lax.rem(me, 2)
    cross = lax.rem(me + 2, 4)
    diag = lax.rem(side + 2, 4)
    pairs = rows // 2
    lat = kvbuf.shape[2]
    rope = kr_hbm.shape[1]
    group = qbuf.shape[2]
    queries = 4 * group

    def to(dev):
        return {"seq": dev}

    def kv_copies(row, slot):
        return (pltpu.make_async_copy(kv_hbm.at[row], kvbuf.at[slot], kv_sem.at[slot]),
                pltpu.make_async_copy(kr_hbm.at[row], krbuf.at[slot, pl.ds(pl.multiple_of(slot * rope, rope), rope)], kr_sem.at[slot]))

    def local_q(k):
        return pltpu.make_async_copy(q_hbm.at[k], qbuf.at[k, 0], q_local.at[k])

    def cross_q(k):
        return pltpu.make_async_remote_copy(q_hbm.at[k], qbuf.at[k, 1], q_cross.at[0, k], q_cross.at[1, k],
                                            device_id=to(cross), device_id_type=MESH)

    def side_q(k):
        return pltpu.make_async_remote_copy(q_hbm.at[k], qbuf.at[k, 2], q_side.at[0, k], q_side.at[1, k],
                                            device_id=to(side), device_id_type=MESH)

    def fwd_q(k):
        return pltpu.make_async_remote_copy(qbuf.at[k, 1], qbuf.at[k, 3], q_fwd.at[0, k], q_fwd.at[1, k],
                                            device_id=to(side), device_id_type=MESH)

    def side_o(row):
        slot, land = lax.rem(row, 2), lax.rem(row, 4)
        return (pltpu.make_async_remote_copy(oacc.at[slot, pl.ds(2 * group, 2 * group)], pbuf.at[land], p_sem.at[0, slot], p_sem.at[1, land],
                                             device_id=to(side), device_id_type=MESH),
                pltpu.make_async_remote_copy(ostat.at[slot, :, pl.ds(2 * group, 2 * group)], pstat.at[land], ps_sem.at[0, slot], ps_sem.at[1, land],
                                             device_id=to(side), device_id_type=MESH))

    def cross_o(row):
        return (pltpu.make_async_remote_copy(xsend.at[row], xrecv.at[row], x_sem.at[0, row], x_sem.at[1, row],
                                             device_id=to(cross), device_id_type=MESH),
                pltpu.make_async_remote_copy(xstat.at[row], xrstat.at[row], xs_sem.at[0, row], xs_sem.at[1, row],
                                             device_id=to(cross), device_id_type=MESH))

    for copy in kv_copies(0, 0):
        copy.start()
    local_q(0).start()
    barrier = pltpu.get_barrier_semaphore()
    for dev in (side, cross, diag):
        pl.semaphore_signal(barrier, inc=1, device_id=to(dev), device_id_type=MESH)
    pl.semaphore_wait(barrier, 3)

    def launch(k, carry):
        cross_q(k).start()
        side_q(k).start()

        @pl.when(k > 0)
        def _():
            local_q(k).start()
        return carry
    lax.fori_loop(0, pairs, launch, 0)
    krbuf[0, rope:, :] = jnp.zeros((rope, krbuf.shape[2]), krbuf.dtype)
    krbuf[1, :rope, :] = jnp.zeros((rope, krbuf.shape[2]), krbuf.dtype)

    def forward(k):
        cross_q(k).wait_recv()
        fwd_q(k).start()

    forward(0)
    fold = score_scale * math.log2(math.e)
    tok_of = lax.rem(lax.broadcasted_iota(jnp.int32, (queries, 1), 0), toks)
    lane_of = lax.broadcasted_iota(jnp.int32, (queries, CHUNK), 1)

    def attend(row, slot):
        pair = row // 2
        q_lat = qbuf[pair, :, :, pl.ds(pl.multiple_of(slot * lat, lat), lat)].reshape(queries, lat)
        q_rot = qbuf[pair, :, :, 2 * lat:].reshape(queries, 2 * rope)
        limit = lens_ref[row] - me * seq_len + tok_of
        top = total = acc = None
        for j in range(seq_len // CHUNK):
            part = kvbuf[slot, j * CHUNK:(j + 1) * CHUNK, :]
            s = lax.dot_general(q_lat, part, (((1,), (1,)), ((), ())), preferred_element_type=jnp.float32)
            s = s + jnp.dot(q_rot, krbuf[slot, :, j * CHUNK:(j + 1) * CHUNK], preferred_element_type=jnp.float32)
            s = jnp.where(lane_of <= limit - j * CHUNK, s * fold, MASK_FILL)
            peak = jnp.max(s, axis=1, keepdims=True)
            new_top = peak if top is None else jnp.maximum(top, peak)
            p = jnp.exp2(s - new_top)
            psum = jnp.sum(p, axis=1, keepdims=True)
            o = jnp.dot(p.astype(jnp.bfloat16), part, preferred_element_type=jnp.float32)
            if top is None:
                total, acc = psum, o
            else:
                keep = jnp.exp2(top - new_top)
                total = total * keep + psum
                acc = acc * keep + o
            top = new_top
        oacc[slot] = acc
        ostat[slot, 0] = jnp.broadcast_to(top, (queries, 128))
        ostat[slot, 1] = jnp.broadcast_to(total, (queries, 128))

    def merge_side(row):
        slot, land = lax.rem(row, 2), lax.rem(row, 4)
        for copy in side_o(row):
            copy.wait()
        top_a, top_b = ostat[slot, 0, :2 * group], pstat[land, 0]
        new_top = jnp.maximum(top_a, top_b)
        keep_a, keep_b = jnp.exp2(top_a - new_top), jnp.exp2(top_b - new_top)
        total = ostat[slot, 1, :2 * group] * keep_a + pstat[land, 1] * keep_b
        for n in range(lat // 128):
            cols = slice(n * 128, (n + 1) * 128)
            merged = oacc[slot, :2 * group, cols] * keep_a + pbuf[land, :, cols] * keep_b
            own[row, :, cols] = merged[:group]
            xsend[row, :, cols] = merged[group:]
        lane = lax.broadcasted_iota(jnp.int32, (2 * group, 128), 1)
        packed = jnp.transpose(jnp.where(lane == 0, new_top, total))
        xstat[row] = packed[:8]
        for copy in cross_o(row):
            copy.start()

    def body(row, carry):
        slot = lax.rem(row, 2)
        pair = row // 2

        @pl.when(row + 1 < rows)
        def _():
            for copy in kv_copies(row + 1, 1 - slot):
                copy.start()

        @pl.when(slot == 0)
        def _():
            local_q(pair).wait()
            side_q(pair).wait_recv()
            fwd_q(pair).wait_recv()

        @pl.when((slot == 1) & (pair + 1 < pairs))
        def _():
            forward(pair + 1)

        for copy in kv_copies(row, slot):
            copy.wait()
        attend(row, slot)
        for copy in side_o(row):
            copy.start()

        @pl.when(row > 0)
        def _():
            merge_side(row - 1)
        return carry

    lax.fori_loop(0, rows, body, 0)
    merge_side(rows - 1)

    def finish(step, carry):
        parts = []
        for n in range(4):
            row = 4 * step + n
            for copy in cross_o(row):
                copy.wait_recv()
            pad = jnp.zeros((120, 128), jnp.float32)
            mine = jnp.transpose(jnp.concatenate([xstat[row], pad], axis=0))[:group]
            theirs = jnp.transpose(jnp.concatenate([xrstat[row], pad], axis=0))[group:]
            top_a, top_b = mine[:, 0:1], theirs[:, 0:1]
            new_top = jnp.maximum(top_a, top_b)
            keep_a, keep_b = jnp.exp2(top_a - new_top), jnp.exp2(top_b - new_top)
            total = mine[:, 1:2] * keep_a + theirs[:, 1:2] * keep_b
            parts.append(((own[row] * keep_a + xrecv[row] * keep_b) / total).astype(jnp.bfloat16))
        by_row = jnp.concatenate(parts, axis=0)
        dst = lax.broadcasted_iota(jnp.int32, (4 * group, 4 * group), 0)
        src = lax.broadcasted_iota(jnp.int32, (4 * group, 4 * group), 1)
        head, rest = dst // (4 * toks), lax.rem(dst, 4 * toks)
        wanted = (rest // toks) * group + head * toks + lax.rem(rest, toks)
        pick = jnp.where(src == wanted, 1.0, 0.0).astype(jnp.bfloat16)
        by_head = jnp.dot(pick, by_row, preferred_element_type=jnp.float32).astype(jnp.bfloat16)
        o_ref[:, pl.ds(pl.multiple_of(step * 4 * toks, 4 * toks), 4 * toks), :] = by_head.reshape(group // toks, 4 * toks, lat)
        return carry
    lax.fori_loop(0, rows // 4, finish, 0)

    def drain_q(k, carry):
        cross_q(k).wait_send()
        side_q(k).wait_send()
        fwd_q(k).wait_send()
        return carry
    lax.fori_loop(0, pairs, drain_q, 0)

    def drain_o(row, carry):
        for copy in cross_o(row):
            copy.wait_send()
        return carry
    lax.fori_loop(0, rows, drain_o, 0)


def _attend(lens, q_pack, c_kv, k_rt, toks, score_scale):
    rows, seq_len, lat = c_kv.shape
    rope = k_rt.shape[1]
    pairs, group, width = q_pack.shape
    f32, bf16 = jnp.float32, jnp.bfloat16
    dma = pltpu.SemaphoreType.DMA
    return pl.pallas_call(
        functools.partial(_attend_kernel, rows, toks, seq_len, score_scale),
        out_shape=jax.ShapeDtypeStruct((group // toks, rows * toks, lat), bf16),
        in_specs=[pl.BlockSpec(memory_space=pltpu.SMEM)] + [pl.BlockSpec(memory_space=pl.ANY)] * 3,
        out_specs=pl.BlockSpec(memory_space=pltpu.VMEM),
        scratch_shapes=[
            pltpu.VMEM((pairs, 4, group, width), bf16),
            pltpu.VMEM((2, seq_len, lat), bf16),
            pltpu.VMEM((2, 2 * rope, seq_len), bf16),
            pltpu.VMEM((2, 4 * group, lat), f32),
            pltpu.VMEM((2, 2, 4 * group, 128), f32),
            pltpu.VMEM((4, 2 * group, lat), f32),
            pltpu.VMEM((4, 2, 2 * group, 128), f32),
            pltpu.VMEM((rows, group, lat), f32),
            pltpu.VMEM((rows, 8, 128), f32),
            pltpu.VMEM((rows, group, lat), f32),
            pltpu.VMEM((rows, 8, 128), f32),
            pltpu.VMEM((rows, group, lat), f32),
            dma((pairs,)), dma((2, pairs)), dma((2, pairs)), dma((2, pairs)),
            dma((2,)), dma((2,)), dma((2, 4)), dma((2, 4)), dma((2, rows)), dma((2, rows)),
        ],
        compiler_params=pltpu.CompilerParams(collective_id=0, has_side_effects=True, vmem_limit_bytes=60 * 1024 * 1024),
        name="attend",
    )(lens, q_pack, c_kv, k_rt)


def _project_kernel(chunks, o_ref, wuv_ref, hid_ref, wo_hbm, out_ref, ov, rel, hrel, wbuf, ybuf, sbuf, ybin, xbuf, fin,
                    w_sem, s_sem, x_sem, b_sem, c_sem, f_sem):
    me = lax.axis_index("seq")
    side = me + 1 - 2 * lax.rem(me, 2)
    cross = lax.rem(me + 2, 4)
    diag = lax.rem(side + 2, 4)
    heads = o_ref.shape[0]
    tokens = o_ref.shape[1]
    val = wuv_ref.shape[2]
    part = tokens // 4
    width = wbuf.shape[2]
    toks = out_ref.shape[1]

    def to(dev):
        return {"seq": dev}

    def fetch(j):
        return pltpu.make_async_copy(wo_hbm.at[:, pl.ds(j * width, width)], wbuf.at[j], w_sem.at[j])

    def side_y(j):
        return pltpu.make_async_remote_copy(ybuf.at[j, pl.ds(2 * part, 2 * part)], sbuf.at[j], s_sem.at[0, j], s_sem.at[1, j],
                                            device_id=to(side), device_id_type=MESH)

    def cross_y(j):
        return pltpu.make_async_remote_copy(ybin.at[j], xbuf.at[j], x_sem.at[0, j], x_sem.at[1, j],
                                            device_id=to(cross), device_id_type=MESH)

    def side_fin(j):
        return pltpu.make_async_remote_copy(fin.at[j, 0], fin.at[j, 2], b_sem.at[0, j], b_sem.at[1, j],
                                            device_id=to(side), device_id_type=MESH)

    def cross_fin(j):
        return pltpu.make_async_remote_copy(fin.at[j, 0], fin.at[j, 1], c_sem.at[0, j], c_sem.at[1, j],
                                            device_id=to(cross), device_id_type=MESH)

    def fwd_fin(j):
        return pltpu.make_async_remote_copy(fin.at[j, 1], fin.at[j, 3], f_sem.at[0, j], f_sem.at[1, j],
                                            device_id=to(side), device_id_type=MESH)

    for j in range(chunks):
        fetch(j).start()
    barrier = pltpu.get_barrier_semaphore()
    for dev in (side, cross, diag):
        pl.semaphore_signal(barrier, inc=1, device_id=to(dev), device_id_type=MESH)
    for h in range(heads):
        ov[:, h * val:(h + 1) * val] = jnp.dot(o_ref[h], wuv_ref[h], preferred_element_type=jnp.float32).astype(jnp.bfloat16)
    for n, dev in enumerate((me, cross, side, diag)):
        rows_of = pl.ds(pl.multiple_of(dev * part, part), part)
        rel[n * part:(n + 1) * part, :] = ov[rows_of, :]
    hrel[...] = hid_ref[pl.ds(pl.multiple_of(me * part, part), part), :]
    pl.semaphore_wait(barrier, 3)

    def stage_sum(j):
        side_y(j).wait_recv()
        both = ybuf[j, :2 * part] + sbuf[j]
        ybuf[j, :part] = both[:part]
        ybin[j] = both[part:]
        cross_y(j).start()

    def stage_fin(j):
        cross_y(j).wait_recv()
        cols = slice(j * width, (j + 1) * width)
        y = ybuf[j, :part] + xbuf[j]
        fin[j, 0] = (hrel[:, cols].astype(jnp.float32) + y).astype(jnp.bfloat16)
        side_fin(j).start()
        cross_fin(j).start()

    def stage_fwd(j):
        cross_fin(j).wait_recv()
        fwd_fin(j).start()

    def stage_out(j):
        side_fin(j).wait_recv()
        fwd_fin(j).wait_recv()
        cols = slice(j * width, (j + 1) * width)
        for n, dev in enumerate((me, cross, side, diag)):
            block = fin[j, n].reshape(part // toks, toks, width)
            out_ref[pl.ds(dev * (part // toks), part // toks), :, cols] = block

    for j in range(chunks + 5):
        if j < chunks:
            fetch(j).wait()
            ybuf[j] = jnp.dot(rel[...], wbuf[j], preferred_element_type=jnp.float32)
            side_y(j).start()
        if 1 <= j <= chunks:
            stage_sum(j - 1)
        if 3 <= j < chunks + 3:
            stage_fin(j - 3)
        if 4 <= j < chunks + 4:
            stage_fwd(j - 4)
        if j >= 5:
            stage_out(j - 5)
    for j in range(chunks):
        side_y(j).wait_send()
        cross_y(j).wait_send()
        side_fin(j).wait_send()
        cross_fin(j).wait_send()
        fwd_fin(j).wait_send()


def _project(o_lat, w_uv, hidden, w_o, chunks):
    rows, toks, model = hidden.shape
    heads, tokens, lat = o_lat.shape
    depth = w_o.shape[0]
    width = model // chunks
    part = tokens // 4
    f32, bf16 = jnp.float32, jnp.bfloat16
    dma = pltpu.SemaphoreType.DMA
    vmem = pl.BlockSpec(memory_space=pltpu.VMEM)
    return pl.pallas_call(
        functools.partial(_project_kernel, chunks),
        out_shape=jax.ShapeDtypeStruct((rows, toks, model), bf16),
        in_specs=[vmem, vmem, vmem, pl.BlockSpec(memory_space=pl.ANY)],
        out_specs=vmem,
        scratch_shapes=[
            pltpu.VMEM((tokens, depth), bf16),
            pltpu.VMEM((tokens, depth), bf16),
            pltpu.VMEM((part, model), bf16),
            pltpu.VMEM((chunks, depth, width), bf16),
            pltpu.VMEM((chunks, tokens, width), f32),
            pltpu.VMEM((chunks, 2 * part, width), f32),
            pltpu.VMEM((chunks, part, width), f32),
            pltpu.VMEM((chunks, part, width), f32),
            pltpu.VMEM((chunks, 4, part, width), bf16),
            dma((chunks,)), dma((2, chunks)), dma((2, chunks)), dma((2, chunks)), dma((2, chunks)), dma((2, chunks)),
        ],
        compiler_params=pltpu.CompilerParams(collective_id=1, has_side_effects=True, vmem_limit_bytes=60 * 1024 * 1024),
        name="project",
    )(o_lat, w_uv, hidden.reshape(tokens, model), w_o)


def solution(mesh):
    def local_step(hidden, cache_lens, c_kv, k_r, w_uq, w_qr, w_uk, w_uv, w_o):
        rows, toks, _ = hidden.shape
        heads, nope, lat = w_uk.shape
        rope = w_qr.shape[2]
        score_scale = (nope + rope) ** -0.5
        q_nope = jnp.einsum("cre,eil->cril", hidden, w_uq, preferred_element_type=jnp.float32).astype(jnp.bfloat16)
        q_rope = jnp.einsum("cre,eis->cris", hidden, w_qr, preferred_element_type=jnp.float32).astype(jnp.bfloat16)
        q_lat = jnp.einsum("bqhk,hkc->bqhc", q_nope, w_uk, preferred_element_type=jnp.float32).astype(jnp.bfloat16)
        q_lat = q_lat.reshape(rows // 2, 2, toks, heads, lat).transpose(0, 3, 2, 1, 4).reshape(rows // 2, heads * toks, 2 * lat)
        q_rope = q_rope.reshape(rows // 2, 2, toks, heads, rope).transpose(0, 3, 2, 1, 4).reshape(rows // 2, heads * toks, 2 * rope)
        q_pack = jnp.concatenate([q_lat, q_rope], axis=-1)
        o_lat = _attend(cache_lens, q_pack, c_kv, jnp.swapaxes(k_r, 1, 2), toks, score_scale)
        return _project(o_lat, w_uv, hidden, w_o.reshape(-1, w_o.shape[2]), 12)

    specs_in = (P("batch", None, None), P("batch"), P("batch", "seq", None), P("batch", "seq", None),
                P(None, "seq", None), P(None, "seq", None), P("seq", None, None), P("seq", None, None),
                P("seq", None, None))
    return jax.shard_map(local_step, mesh=mesh, in_specs=specs_in, out_specs=P("batch", None, None), check_vma=False)
```
